512 devices in a mesh: group: 2 (over y), seq: 32 (over z), head: 4 (over x), sub: 2 (over core).
Axes of the slice: x: 4, y: 2, z: 32, core: 2. Of those that a mesh axis runs over, the one named last changes fastest.
The devices are a block of a 4x8x32 slice.
Arguments:
- queries: bfloat16 [32, 32, 128], P(('group', 'sub'), 'head'), parts along dimension 0, may hold values from -8 to 8
- lengths: int32 [32], P(('group', 'sub')), parts along dimension 0, may hold values from 1 to 192, 2048 in all
- k_cache: bfloat16 [524288, 8, 128], P(('group', 'seq', 'sub'), 'head'), parts along dimension 0, may hold values from -12 to 12
- v_cache: bfloat16 [524288, 8, 128], P(('group', 'seq', 'sub'), 'head'), parts along dimension 0, may hold values from -6 to 6
Outputs:
- attended: bfloat16 [32, 32, 128], P('group', ('head', 'sub')), parts along dimension 0
The draws below stay inside these ranges and needn't reach their ends.
There are 2 independent parts, one for each index of `group`. The reference program is written for one: setup_inputs(seed, part) draws one part's arguments, and reference() takes and returns one part's arrays. A program takes and returns all parts, laid end to end along the dimension named above; each array names one. Nothing has to cross between parts.
Inputs may be any that keep to these rules, and one draw needn't show every extreme that they name: The lengths sum to exactly 2048, and some request has exactly 192 pages.
All inputs are finite; a program needn't handle non-finite values. No bound on the sum of `lengths` on one device may be relied on, other than what follows from the above.
Results may differ from the reference program's by a relative error of at most 0.0044.
Values may be sent and summed in bfloat16 or wider, within the bound.
A program may use at most 64 MiB of HBM per device.

```python
import math
import jax
import jax.numpy as jnp
import numpy as np
from jax import lax

QH = 32
KVH = 8
HD = 128
PAGE = 128
R = 16
TOTAL_PAGES = 2048
TOKENS = 262144
MOST = 192


def draw_queries(key, part):
    noise = jnp.clip(jax.random.normal(jax.random.fold_in(key, 11), (R, QH, HD), jnp.float32), -6.0, 6.0)
    values = noise
    return values.astype(jnp.bfloat16)


def draw_k_cache(key, part):
    noise = jnp.clip(jax.random.normal(jax.random.fold_in(key, 17), (TOKENS, KVH, HD), jnp.float32), -6.0, 6.0)
    values = noise
    return values.astype(jnp.bfloat16)


def shard_levels(own_key, dims, shards, low, high):
    factor_of = 1.0
    for dim, blocks in shards:
        draws = jax.random.uniform(jax.random.fold_in(jax.random.fold_in(own_key, 6), dim), (blocks,), jnp.float32, low / len(shards), high / len(shards))
        factor_of = factor_of * jnp.repeat(jnp.exp(draws), dims[dim] // blocks).reshape((-1,) + (1,) * (len(dims) - 1 - dim))
    return factor_of


def split_up(count, total, reach, skew):
    portions = [(1 << 20) // math.isqrt(grade ** skew) + 1 for grade in range(2, count + 1)]
    surplus, holding = total - reach - (count - 1), [1] * (count - 1)
    while surplus > 0:
        free = [i for i in range(count - 1) if holding[i] < reach]
        mass, remaining = sum([portions[i] for i in free]), surplus
        for i in free:
            addition = min(reach - holding[i], max(1, remaining * portions[i] // mass), surplus)
            holding[i] = holding[i] + addition
            surplus = surplus - addition
    return np.array([reach] + holding)


def uneven_parts(rng, number_of, total, reach, slope):
    if number_of == 2:
        one = jax.random.randint(rng, (), max(1, total - reach), min(reach, total - 1) + 1)
        return jnp.stack([one, total - one])
    tallies = jnp.asarray(split_up(number_of, total, reach, slope), jnp.int32)
    twos = (number_of - 1) // 2
    source_of, receiver = tallies[1:1 + 2 * twos:2], tallies[2:2 + 2 * twos:2]
    slack = jnp.minimum(source_of - 1, reach - receiver)
    moved = jax.random.randint(jax.random.fold_in(rng, 1), (twos,), 0, 1 << 20) % (slack + 1)
    tallies = tallies.at[1:1 + 2 * twos:2].set(source_of - moved).at[2:2 + 2 * twos:2].set(receiver + moved)
    return tallies[jax.random.permutation(jax.random.fold_in(rng, 2), number_of)]


def centred(key, dims, deviation, most, shards=(), kind=jnp.bfloat16):
    array = deviation * jax.random.normal(key, dims, jnp.float32)
    if shards:
        array = array * shard_levels(key, dims, shards, -0.22, 0.18)
    return jnp.clip(array, -most, most).astype(kind)


def setup_inputs(seed: int = 0, part: int = 0) -> dict:
    key_of = jax.random.split(jax.random.key(seed), 5)
    part_keys = jax.random.split(jax.random.fold_in(key_of[4], part), 5)
    queries = draw_queries(jax.random.fold_in(jax.random.fold_in(key_of[4], part), 71), part)
    lengths = uneven_parts(part_keys[1], R, TOTAL_PAGES, MOST, 2).astype(jnp.int32)
    k_cache = draw_k_cache(jax.random.fold_in(jax.random.fold_in(key_of[4], part), 71), part)
    v_cache = centred(part_keys[3], (TOKENS, KVH, HD), 1.0, 6.0, ((0, 64), (1, 4)))
    return {"queries": queries, "lengths": lengths, "k_cache": k_cache, "v_cache": v_cache}


lowest_score = -1e30


def reference(queries, lengths, k_cache, v_cache):
    request_count = queries.shape[0]
    query_heads = queries.shape[1]
    head_width = queries.shape[2]
    key_heads = k_cache.shape[1]
    group_size = query_heads // key_heads
    page_count = k_cache.shape[0] // PAGE
    scale = float(head_width) ** -0.5
    starts = (jnp.cumsum(lengths) - lengths).astype(jnp.int32)
    page_ids = jnp.arange(page_count, dtype=jnp.int32)
    owner = (jnp.sum((starts[None, :] <= page_ids[:, None]).astype(jnp.int32), axis=1) - 1).astype(jnp.int32)
    page_query = jnp.take(queries, owner, axis=0).reshape(page_count, key_heads, group_size, head_width)
    key_pages = k_cache.reshape(page_count, PAGE, key_heads, head_width)
    value_pages = v_cache.reshape(page_count, PAGE, key_heads, head_width)
    block = math.gcd(64, page_count)
    blocks = page_count // block

    def one_block(pieces):
        query_block, key_block, value_block = pieces
        scores = jnp.einsum("pskd,pkgd->pkgs", key_block.astype(jnp.float32), query_block.astype(jnp.float32)) * scale
        page_max = jnp.max(scores, axis=3)
        weights = jnp.exp(scores - page_max[..., None])
        page_sum = jnp.sum(weights, axis=3)
        rounded = lax.optimization_barrier(weights.astype(jnp.bfloat16)).astype(jnp.float32)
        page_out = jnp.einsum("pkgs,pskd->pkgd", rounded, value_block.astype(jnp.float32))
        return page_max, page_sum, page_out

    page_max, page_sum, page_out = lax.map(one_block, (
        page_query.reshape(blocks, block, key_heads, group_size, head_width),
        key_pages.reshape(blocks, block, PAGE, key_heads, head_width),
        value_pages.reshape(blocks, block, PAGE, key_heads, head_width)))
    page_max = page_max.reshape(page_count, key_heads, group_size)
    page_sum = page_sum.reshape(page_count, key_heads, group_size)
    page_out = page_out.reshape(page_count, key_heads, group_size, head_width)
    member = owner[:, None] == jnp.arange(request_count, dtype=jnp.int32)[None, :]
    request_max = jnp.max(jnp.where(member[:, :, None, None], page_max[:, None], lowest_score), axis=0)
    rescale = jnp.exp(page_max - jnp.take(request_max, owner, axis=0))
    numer = jax.ops.segment_sum(rescale[..., None] * page_out, owner, num_segments=request_count)
    denom = jax.ops.segment_sum(rescale * page_sum, owner, num_segments=request_count)
    attended = numer / denom[..., None]
    return attended.reshape(request_count, query_heads, head_width).astype(jnp.bfloat16)
```

```python
import functools

import jax
import jax.numpy as jnp
from jax import lax
from jax.experimental import pallas as pl
from jax.experimental.pallas import tpu as pltpu
from jax.sharding import PartitionSpec as P

PAGE = 128
LONGEST = 192
CORES = 2
NEG = -1e30
MESH = pl.DeviceIdType.MESH
PARTS = 4


def kernel(
    chips,
    q_hbm,
    len_hbm,
    k_hbm,
    v_hbm,
    out_ref,
    kbuf,
    vbuf,
    qbuf,
    score,
    weight,
    run_max,
    run_sum,
    run_out,
    sent,
    got,
    final,
    len_vm,
    len_sm,
    start_sm,
    k_sem,
    v_sem,
    in_sem,
    x_send,
    x_recv,
    token,
    r_send,
    r_recv,
    g_send,
    g_recv,
):
    c, s = lax.axis_index("seq"), lax.axis_index("sub")
    own_requests, heads, width = q_hbm.shape
    requests = own_requests * CORES
    group = heads // CORES
    rows = kbuf.shape[0]
    pages = rows // (PAGE * CORES)
    page_rows = PAGE * CORES
    chunks = k_sem.shape[0]
    chunk_rows = rows // chunks
    chunk_pages = pages // chunks
    per_part = requests // PARTS
    reach = got.shape[0] // (2 * CORES)
    far = chips // 4

    def chip(offset):
        return lax.rem(c + (offset + chips), chips)

    def at(offset, core):
        return {"seq": chip(offset), "sub": core}

    barrier = pltpu.get_barrier_semaphore()
    near = [(o, k) for o in (1, -1) for k in range(CORES)]
    for o, k in near:
        pl.semaphore_signal(barrier, inc=1, device_id=at(o, k), device_id_type=MESH)
    pl.semaphore_signal(barrier, inc=1, device_id=at(0, 1 - s), device_id_type=MESH)

    def k_copy(i):
        part = pl.ds(i * chunk_rows, chunk_rows)
        return pltpu.make_async_copy(k_hbm.at[part], kbuf.at[part], k_sem.at[i])

    def v_copy(i):
        part = pl.ds(i * chunk_rows, chunk_rows)
        return pltpu.make_async_copy(v_hbm.at[part], vbuf.at[part], v_sem.at[i])

    own = pl.ds(s * own_requests, own_requests)
    q_own = pltpu.make_async_copy(q_hbm, qbuf.at[own], in_sem.at[0])
    l_own = pltpu.make_async_copy(len_hbm, len_vm.at[s], in_sem.at[1])
    q_own.start()
    l_own.start()
    for i in range(chunks):
        k_copy(i).start()
    for i in range(chunks):
        v_copy(i).start()

    pl.semaphore_wait(barrier, len(near) + 1)
    q_away = pltpu.make_async_remote_copy(
        src_ref=q_hbm, dst_ref=qbuf.at[own], send_sem=x_send.at[0], recv_sem=x_recv.at[0],
        device_id=at(0, 1 - s), device_id_type=MESH,
    )
    l_away = pltpu.make_async_remote_copy(
        src_ref=len_hbm, dst_ref=len_vm.at[s], send_sem=x_send.at[1], recv_sem=x_recv.at[1],
        device_id=at(0, 1 - s), device_id_type=MESH,
    )
    l_away.start()
    q_away.start()

    def signal_level(level):
        for side, o in enumerate((1 << level, -(1 << level))):
            pl.semaphore_signal(token.at[level, side], inc=1, device_id=at(o, s), device_id_type=MESH)

    def wait_level(level):
        for side in range(2):
            pl.semaphore_wait(token.at[level, side], 1)

    signal_level(0)

    l_own.wait()
    l_away.wait()
    l_down = pltpu.make_async_copy(len_vm, len_sm, in_sem.at[2])
    l_down.start()
    l_down.wait()
    starts = []
    total = jnp.int32(0)
    for r in range(requests):
        starts.append(total)
        start_sm[r] = total
        total = total + len_sm[r // own_requests, r % own_requests]
    start_sm[requests] = total
    base = (c * CORES + s) * pages
    owner = jnp.int32(-1)
    for r in range(requests):
        owner = owner + (starts[r] <= base).astype(jnp.int32)
    owners, firsts = [owner], [None]
    for p in range(1, pages):
        begins = start_sm[owner + 1] <= base + p
        owner = jnp.minimum(owner + begins.astype(jnp.int32), requests - 1)
        owners.append(owner)
        firsts.append(begins)

    q_own.wait()
    q_away.wait()
    lane_head = lax.rem(lax.broadcasted_iota(jnp.int32, (heads, page_rows), 1), CORES)
    row_head = lax.broadcasted_iota(jnp.int32, (heads, page_rows), 0) // group
    mine = lane_head == row_head
    scale = float(width) ** -0.5
    running = None
    for p in range(pages):
        if p % chunk_pages == 0:
            k_copy(p // chunk_pages).wait()
        keys = kbuf[p * page_rows : (p + 1) * page_rows, :]
        values = lax.dot_general(
            qbuf[owners[p]], keys, (((1,), (1,)), ((), ())), preferred_element_type=jnp.float32
        )
        values = jnp.where(mine, values * scale, NEG)
        score[p] = values
        top = jnp.broadcast_to(jnp.max(values, axis=1, keepdims=True), (heads, width))
        running = top if p == 0 else jnp.where(firsts[p], top, jnp.maximum(running, top))
        run_max[p] = running

    wait_level(0)
    signal_level(1)

    running = None
    for p in range(pages):
        last = jnp.clip(start_sm[owners[p] + 1] - base - 1, 0, pages - 1)
        peak = run_max[last].astype(jnp.bfloat16).astype(jnp.float32)
        half = jnp.exp(score[p] - jnp.concatenate([peak] * CORES, axis=1)).astype(jnp.bfloat16)
        weight[p] = half
        added = jnp.broadcast_to(
            jnp.sum(half.astype(jnp.float32), axis=1, keepdims=True), (heads, width)
        )
        running = added if p == 0 else jnp.where(firsts[p], added, running + added)
        run_sum[p] = running

    running = None
    for p in range(pages):
        if p % chunk_pages == 0:
            v_copy(p // chunk_pages).wait()
        values = vbuf[p * page_rows : (p + 1) * page_rows, :]
        added = jnp.dot(weight[p], values, preferred_element_type=jnp.float32)
        running = added if p == 0 else jnp.where(firsts[p], added, running + added)
        run_out[p] = running

    lane = lax.broadcasted_iota(jnp.int32, (heads, width), 1)
    tops, sums, outs = [], [], []
    for r in range(requests):
        begin = jnp.maximum(starts[r] - base, 0)
        end = jnp.minimum(start_sm[r + 1] - base, pages)
        here = end > begin
        last = jnp.clip(end - 1, 0, pages - 1)
        peak = jnp.where(here, run_max[last], NEG).astype(jnp.bfloat16).astype(jnp.float32)
        weights = jnp.where(here, run_sum[last], 0.0)
        high = weights.astype(jnp.bfloat16).astype(jnp.float32)
        tops.append(jnp.where(lane < 32, peak, jnp.where(lane < 64, high, weights - high)))
        outs.append(jnp.where(here, run_out[last], 0.0))

    for j in range(PARTS):
        members = range(j * per_part, (j + 1) * per_part)
        for k in range(CORES):
            cut = slice(k * group, (k + 1) * group)
            numbers = jnp.concatenate([outs[r][cut] for r in members], axis=0)
            stats = jnp.concatenate([tops[r][cut] for r in members], axis=0)
            sent[j, k] = jnp.concatenate([numbers, stats], axis=0).astype(jnp.bfloat16)

    wait_level(1)
    signal_level(2)

    part_rows = per_part * group
    offsets = [o for n in range(reach, 0, -1) for o in (n, -n)] + [0]

    def part_copy(o, k, n):
        return pltpu.make_async_remote_copy(
            src_ref=sent.at[lax.rem(chip(o), PARTS), k],
            dst_ref=got.at[(reach - o) * CORES + s],
            send_sem=r_send.at[n],
            recv_sem=r_recv.at[(reach - o) * CORES + s],
            device_id=at(o, k),
            device_id_type=MESH,
        )

    def part_arrival(o, k):
        slot = (reach + o) * CORES + k
        return pltpu.make_async_remote_copy(
            src_ref=sent.at[0, 0], dst_ref=got.at[slot], send_sem=r_send.at[0], recv_sem=r_recv.at[slot],
            device_id=at(0, 1 - s), device_id_type=MESH,
        )

    part_copies = []
    for o in offsets:
        for k in range(CORES) if o else (1 - s,):
            part_copies.append(part_copy(o, k, len(part_copies)))
            part_copies[-1].start()
    got[reach * CORES + s] = sent[lax.rem(c, PARTS), s]
    for o in offsets:
        for k in range(CORES) if o else (1 - s,):
            part_arrival(o, k).wait_recv()

    slots = got.shape[0]
    stats = [got[i, part_rows:, :].astype(jnp.float32) for i in range(slots)]
    peak = functools.reduce(jnp.maximum, stats)
    numer, denom = 0.0, 0.0
    for i in range(slots):
        lift = jnp.exp(stats[i][:, 0:1] - peak[:, 0:1])
        numer = numer + lift * got[i, :part_rows, :].astype(jnp.float32)
        denom = denom + lift * stats[i]
    denom = denom[:, 32:33] + denom[:, 64:65]
    denom = jnp.where(denom > 0.0, denom, 1.0)
    final[c] = (numer / denom).astype(jnp.bfloat16)

    spread = []

    def pass_on(origin, o):
        cp = pltpu.make_async_remote_copy(
            src_ref=final.at[origin], dst_ref=final.at[origin], send_sem=g_send.at[len(spread)],
            recv_sem=g_recv.at[origin], device_id=at(o, s), device_id_type=MESH,
        )
        spread.append((origin, o))
        cp.start()

    def spread_copy(n, origin, o):
        return pltpu.make_async_remote_copy(
            src_ref=final.at[origin], dst_ref=final.at[origin], send_sem=g_send.at[n],
            recv_sem=g_recv.at[origin], device_id=at(o, s), device_id_type=MESH,
        )

    known = 1 << 2
    for n in range(1, known + 1):
        for o in (n, -n):
            pass_on(c, o)
    wait_level(2)
    for n in range(known + 1, far + 1):
        for o in (n, -n):
            pass_on(c, o)

    direct = len(spread)

    def upward():
        below = chip(-far)
        spread_copy(0, below, 1).wait_recv()
        for n in range(1, far + 1):
            spread_copy(direct + n - 1, below, n).start()

    def downward():
        above = chip(far)
        spread_copy(0, above, 1).wait_recv()
        for n in range(1, far):
            spread_copy(direct + far + n - 1, above, -n).start()

    @pl.when(c < chips // 2)
    def _():
        downward()
        upward()

    @pl.when(c >= chips // 2)
    def _():
        upward()
        downward()

    for n in range(1, chips):
        if n not in (far, chips - far):
            spread_copy(0, chip(n), 1).wait_recv()

    row_request = lax.broadcasted_iota(jnp.int32, (part_rows, width), 0) // group
    for j in range(PARTS):
        block = None
        for i in range(per_part):
            home = starts[j * per_part + i] // (pages * CORES)
            home = home + lax.rem(j - lax.rem(home, PARTS) + PARTS, PARTS)
            piece = final[lax.rem(home, chips)].astype(jnp.float32)
            block = piece if i == 0 else jnp.where(row_request == i, piece, block)
        out_ref[j * part_rows : (j + 1) * part_rows, :] = block.astype(jnp.bfloat16)

    for n in range(len(part_copies)):
        part_copies[n].wait_send()
    for n, (origin, o) in enumerate(spread):
        spread_copy(n, origin, o).wait_send()
    for n in range(1, far + 1):
        spread_copy(direct + n - 1, chip(-far), n).wait_send()
    for n in range(1, far):
        spread_copy(direct + far + n - 1, chip(far), -n).wait_send()


def shards(queries, lengths, k_cache, v_cache):
    chips = lax.axis_size("seq")
    own_requests, heads, width = queries.shape
    tokens, key_heads, _ = k_cache.shape
    requests = own_requests * CORES
    group = heads // key_heads
    rows = tokens * key_heads
    pages = tokens // PAGE
    page_rows = PAGE * key_heads
    span = -(-(LONGEST - 1) // (pages * CORES))
    window = 2 * span + 1
    part_rows = requests // PARTS * group
    chunks = 4
    far = chips // 4
    bf16, f32 = jnp.bfloat16, jnp.float32
    result = pl.pallas_call(
        functools.partial(kernel, chips),
        out_shape=jax.ShapeDtypeStruct((requests * group, width), bf16),
        in_specs=[pl.BlockSpec(memory_space=pl.ANY)] * 4,
        out_specs=pl.BlockSpec(memory_space=pltpu.VMEM),
        scratch_shapes=[
            pltpu.VMEM((rows, width), bf16),
            pltpu.VMEM((rows, width), bf16),
            pltpu.VMEM((requests, heads, width), bf16),
            pltpu.VMEM((pages, heads, page_rows), f32),
            pltpu.VMEM((pages, heads, page_rows), bf16),
            pltpu.VMEM((pages, heads, width), f32),
            pltpu.VMEM((pages, heads, width), f32),
            pltpu.VMEM((pages, heads, width), f32),
            pltpu.VMEM((PARTS, CORES, 2 * part_rows, width), bf16),
            pltpu.VMEM((window * CORES, 2 * part_rows, width), bf16),
            pltpu.VMEM((chips, part_rows, width), bf16),
            pltpu.VMEM((CORES, own_requests), jnp.int32),
            pltpu.SMEM((CORES, own_requests), jnp.int32),
            pltpu.SMEM((requests + 1,), jnp.int32),
            pltpu.SemaphoreType.DMA((chunks,)),
            pltpu.SemaphoreType.DMA((chunks,)),
            pltpu.SemaphoreType.DMA((3,)),
            pltpu.SemaphoreType.DMA((2,)),
            pltpu.SemaphoreType.DMA((2,)),
            pltpu.SemaphoreType.REGULAR((3, 2)),
            pltpu.SemaphoreType.DMA((window * CORES,)),
            pltpu.SemaphoreType.DMA((window * CORES,)),
            pltpu.SemaphoreType.DMA((4 * far,)),
            pltpu.SemaphoreType.DMA((chips,)),
        ],
        compiler_params=pltpu.CompilerParams(collective_id=0, has_side_effects=True),
    )(queries, lengths, k_cache.reshape(rows, width), v_cache.reshape(rows, width))
    return result.reshape(requests, group, width)


def solution(mesh):
    return jax.shard_map(
        shards,
        mesh=mesh,
        in_specs=(
            P(("group", "sub"), "head", None),
            P(("group", "sub")),
            P(("group", "seq", "sub"), "head", None),
            P(("group", "seq", "sub"), "head", None),
        ),
        out_specs=P("group", ("head", "sub"), None),
        check_vma=False,
    )
```

```python
import functools

import jax
import jax.numpy as jnp
from jax import lax
from jax.experimental import pallas as pl
from jax.experimental.pallas import tpu as pltpu
from jax.sharding import PartitionSpec as P

PAGE = 128
LONGEST = 192
CORES = 2
NEG = -1e30
MESH = pl.DeviceIdType.MESH
STEPS = (1, 2, 4, 4)
PARTS = 4


def rounded(x):
    return x.astype(jnp.bfloat16).astype(jnp.float32)


def kernel(
    chips,
    q_hbm,
    len_hbm,
    k_hbm,
    v_hbm,
    out_ref,
    kbuf,
    vbuf,
    qbuf,
    weight,
    page_max,
    page_sum,
    run_max,
    run_sum,
    run_out,
    sent,
    got,
    final,
    len_vm,
    len_sm,
    start_sm,
    k_sem,
    v_sem,
    in_sem,
    x_send,
    x_recv,
    token,
    r_send,
    r_recv,
    g_send,
    h_send,
    g_recv,
):
    c, s = lax.axis_index("seq"), lax.axis_index("sub")
    own_requests, heads, width = q_hbm.shape
    requests = own_requests * CORES
    group = heads // CORES
    rows = kbuf.shape[0]
    pages = rows // (PAGE * CORES)
    page_rows = PAGE * CORES
    chunks = k_sem.shape[0]
    chunk_rows = rows // chunks
    chunk_pages = pages // chunks
    per_part = requests // PARTS
    reach = got.shape[0] // (2 * CORES)
    far = sum(STEPS) + 1

    def chip(offset):
        return lax.rem(c + (offset + chips), chips)

    def at(offset, core):
        return {"seq": chip(offset), "sub": core}

    barrier = pltpu.get_barrier_semaphore()
    near = [(o, k) for o in (1, -1) for k in range(CORES)]
    for o, k in near:
        pl.semaphore_signal(barrier, inc=1, device_id=at(o, k), device_id_type=MESH)
    pl.semaphore_signal(barrier, inc=1, device_id=at(0, 1 - s), device_id_type=MESH)

    def k_copy(i):
        part = pl.ds(i * chunk_rows, chunk_rows)
        return pltpu.make_async_copy(k_hbm.at[part], kbuf.at[part], k_sem.at[i])

    def v_copy(i):
        part = pl.ds(i * chunk_rows, chunk_rows)
        return pltpu.make_async_copy(v_hbm.at[part], vbuf.at[part], v_sem.at[i])

    own = pl.ds(s * own_requests, own_requests)
    l_out = pltpu.make_async_copy(len_hbm, len_vm, in_sem.at[2])
    l_own = pltpu.make_async_copy(len_hbm, len_sm.at[s], in_sem.at[1])
    q_own = pltpu.make_async_copy(q_hbm, qbuf.at[own], in_sem.at[0])
    l_out.start()
    q_own.start()
    l_own.start()
    for i in range(chunks):
        k_copy(i).start()
    l_out.wait()
    q_own.wait()
    pl.semaphore_wait(barrier, len(near) + 1)
    l_away = pltpu.make_async_remote_copy(
        src_ref=len_vm, dst_ref=len_sm.at[s], send_sem=x_send.at[1], recv_sem=x_recv.at[1],
        device_id=at(0, 1 - s), device_id_type=MESH,
    )
    q_away = pltpu.make_async_remote_copy(
        src_ref=qbuf.at[own], dst_ref=qbuf.at[own], send_sem=x_send.at[0], recv_sem=x_recv.at[0],
        device_id=at(0, 1 - s), device_id_type=MESH,
    )
    l_away.start()
    q_away.start()
    for i in range(chunks):
        v_copy(i).start()

    def signal_level(level):
        for side, o in enumerate((STEPS[level], -STEPS[level])):
            pl.semaphore_signal(token.at[level, side], inc=1, device_id=at(o, s), device_id_type=MESH)

    def wait_level(level):
        for side in range(2):
            pl.semaphore_wait(token.at[level, side], 1)

    signal_level(0)

    l_own.wait()
    l_away.wait()
    starts = []
    total = jnp.int32(0)
    for r in range(requests):
        starts.append(total)
        start_sm[r] = total
        total = total + len_sm[r // own_requests, r % own_requests]
    start_sm[requests] = total
    base = (c * CORES + s) * pages
    owner = jnp.int32(-1)
    for r in range(requests):
        owner = owner + (starts[r] <= base).astype(jnp.int32)
    owners, firsts = [owner], [None]
    for p in range(1, pages):
        begins = start_sm[owner + 1] <= base + p
        owner = jnp.minimum(owner + begins.astype(jnp.int32), requests - 1)
        owners.append(owner)
        firsts.append(begins)

    q_away.wait()
    lane_head = lax.rem(lax.broadcasted_iota(jnp.int32, (heads, page_rows), 1), CORES)
    row_head = lax.broadcasted_iota(jnp.int32, (heads, page_rows), 0) // group
    mine = lane_head == row_head
    scale = float(width) ** -0.5
    running = None
    for p in range(pages):
        if p % chunk_pages == 0:
            k_copy(p // chunk_pages).wait()
        keys = kbuf[p * page_rows : (p + 1) * page_rows, :]
        values = lax.dot_general(
            qbuf[owners[p]], keys, (((1,), (1,)), ((), ())), preferred_element_type=jnp.float32
        )
        values = jnp.where(mine, values * scale, NEG)
        top = jnp.broadcast_to(jnp.max(values, axis=1, keepdims=True), (heads, width))
        values = jnp.exp(values - jnp.concatenate([top] * CORES, axis=1))
        weight[p] = values.astype(jnp.bfloat16)
        page_max[p] = top
        page_sum[p] = jnp.broadcast_to(jnp.sum(values, axis=1, keepdims=True), (heads, width))
        running = top if p == 0 else jnp.where(firsts[p], top, jnp.maximum(running, top))
        run_max[p] = running

    wait_level(0)
    signal_level(1)

    summed = gathered = None
    for p in range(pages):
        if p % chunk_pages == 0:
            v_copy(p // chunk_pages).wait()
        last = jnp.clip(start_sm[owners[p] + 1] - base - 1, 0, pages - 1)
        lift = jnp.exp(page_max[p] - rounded(run_max[last]))
        values = vbuf[p * page_rows : (p + 1) * page_rows, :]
        added = lift * jnp.dot(weight[p], values, preferred_element_type=jnp.float32)
        gathered = added if p == 0 else jnp.where(firsts[p], added, gathered + added)
        run_out[p] = gathered
        added = lift * page_sum[p]
        summed = added if p == 0 else jnp.where(firsts[p], added, summed + added)
        run_sum[p] = summed

    lane = lax.broadcasted_iota(jnp.int32, (heads, width), 1)
    half = lax.rem(lane, width // 2)
    tops, sums, outs = [], [], []
    for r in range(requests):
        begin = jnp.maximum(starts[r] - base, 0)
        end = jnp.minimum(start_sm[r + 1] - base, pages)
        here = end > begin
        last = jnp.clip(end - 1, 0, pages - 1)
        peak = rounded(jnp.where(here, run_max[last], NEG))
        weights = jnp.where(here, run_sum[last], 0.0)
        high = weights.astype(jnp.bfloat16).astype(jnp.float32)
        tops.append(jnp.where(half < 16, peak, jnp.where(half < 32, high, weights - high)))
        outs.append(jnp.where(here, run_out[last], 0.0))

    for j in range(PARTS):
        members = range(j * per_part, (j + 1) * per_part)
        for k in range(CORES):
            cut = slice(k * group, (k + 1) * group)
            numbers = jnp.concatenate([outs[r][cut] for r in members], axis=0)
            lower, upper = (
                jnp.concatenate([tops[r][cut] for r in some], axis=0)
                for some in (members[: per_part // 2], members[per_part // 2 :])
            )
            stats = jnp.where(lane < width // 2, lower, upper)
            sent[j, k] = jnp.concatenate([numbers, stats], axis=0).astype(jnp.bfloat16)

    wait_level(1)
    signal_level(2)

    part_rows = per_part * group
    offsets = [o for n in range(reach, 0, -1) for o in (n, -n)] + [0]

    def part_copy(o, k, n):
        return pltpu.make_async_remote_copy(
            src_ref=sent.at[lax.rem(chip(o), PARTS), k],
            dst_ref=got.at[(reach - o) * CORES + s],
            send_sem=r_send.at[n],
            recv_sem=r_recv.at[(reach - o) * CORES + s],
            device_id=at(o, k),
            device_id_type=MESH,
        )

    def part_arrival(o, k):
        slot = (reach + o) * CORES + k
        return pltpu.make_async_remote_copy(
            src_ref=sent.at[0, 0], dst_ref=got.at[slot], send_sem=r_send.at[0], recv_sem=r_recv.at[slot],
            device_id=at(0, 1 - s), device_id_type=MESH,
        )

    part_copies = []
    for o in offsets:
        for k in range(CORES) if o else (1 - s,):
            part_copies.append(part_copy(o, k, len(part_copies)))
            part_copies[-1].start()
    got[reach * CORES + s] = sent[lax.rem(c, PARTS), s]
    wait_level(2)
    signal_level(3)
    for o in offsets:
        for k in range(CORES) if o else (1 - s,):
            part_arrival(o, k).wait_recv()

    slots = got.shape[0]
    stats = [got[i, part_rows:, :].astype(jnp.float32) for i in range(slots)]
    peak = functools.reduce(jnp.maximum, stats)
    blocks = []
    for t in range(2):
        first = t * width // 2
        numer, denom = 0.0, 0.0
        for i in range(slots):
            lift = jnp.exp(stats[i][:, first : first + 1] - peak[:, first : first + 1])
            part = got[i, t * part_rows // 2 : (t + 1) * part_rows // 2, :]
            numer = numer + lift * part.astype(jnp.float32)
            denom = denom + lift * stats[i]
        denom = denom[:, first + 16 : first + 17] + denom[:, first + 32 : first + 33]
        blocks.append(numer / jnp.where(denom > 0.0, denom, 1.0))
    final[c] = jnp.concatenate(blocks, axis=0).astype(jnp.bfloat16)

    def spread_copy(sem, origin, to):
        return pltpu.make_async_remote_copy(
            src_ref=final.at[origin], dst_ref=final.at[origin], send_sem=sem,
            recv_sem=g_recv.at[origin], device_id={"seq": to, "sub": s}, device_id_type=MESH,
        )

    def arrived(origin):
        spread_copy(g_send.at[0], origin, chip(1)).wait_recv()

    wait_level(3)
    beyond = chips // 2 - far
    direct = [o for n in range(1, far + 1) for o in (n, -n)]
    for to in range(chips):
        ahead = lax.rem(to - c + chips, chips)

        @pl.when((ahead > 0) & ((ahead <= far) | (ahead >= chips - far)))
        def _():
            spread_copy(g_send.at[to], c, to).start()

    def upward(act):
        for n in range(1, beyond + 1):
            act(spread_copy(h_send.at[n - 1], chip(-far), chip(n)))

    def downward(act):
        for n in range(1, beyond):
            act(spread_copy(h_send.at[beyond + n - 1], chip(far), chip(-n)))

    @pl.when(c < chips // 2)
    def _():
        arrived(chip(far))
        downward(lambda copy: copy.start())
        arrived(chip(-far))
        upward(lambda copy: copy.start())

    @pl.when(c >= chips // 2)
    def _():
        arrived(chip(-far))
        upward(lambda copy: copy.start())
        arrived(chip(far))
        downward(lambda copy: copy.start())

    for n in range(1, chips):
        if n not in (far, chips - far):
            arrived(chip(n))

    row_request = lax.broadcasted_iota(jnp.int32, (part_rows, width), 0) // group
    for j in range(PARTS):
        block = None
        for i in range(per_part):
            home = starts[j * per_part + i] // (pages * CORES)
            home = home + lax.rem(j - lax.rem(home, PARTS) + PARTS, PARTS)
            piece = final[lax.rem(home, chips)].astype(jnp.float32)
            block = piece if i == 0 else jnp.where(row_request == i, piece, block)
        out_ref[j * part_rows : (j + 1) * part_rows, :] = block.astype(jnp.bfloat16)

    for n in range(len(part_copies)):
        part_copies[n].wait_send()
    for o in direct:
        spread_copy(g_send.at[chip(o)], c, chip(o)).wait_send()
    upward(lambda copy: copy.wait_send())
    downward(lambda copy: copy.wait_send())


def shards(queries, lengths, k_cache, v_cache):
    chips = lax.axis_size("seq")
    own_requests, heads, width = queries.shape
    tokens, key_heads, _ = k_cache.shape
    requests = own_requests * CORES
    group = heads // key_heads
    rows = tokens * key_heads
    pages = tokens // PAGE
    page_rows = PAGE * key_heads
    span = -(-(LONGEST - 1) // (pages * CORES))
    window = 2 * span + 1
    part_rows = requests // PARTS * group
    chunks = 4
    bf16, f32 = jnp.bfloat16, jnp.float32
    result = pl.pallas_call(
        functools.partial(kernel, chips),
        out_shape=jax.ShapeDtypeStruct((requests * group, width), bf16),
        in_specs=[pl.BlockSpec(memory_space=pl.ANY)] * 4,
        out_specs=pl.BlockSpec(memory_space=pltpu.VMEM),
        scratch_shapes=[
            pltpu.VMEM((rows, width), bf16),
            pltpu.VMEM((rows, width), bf16),
            pltpu.VMEM((requests, heads, width), bf16),
            pltpu.VMEM((pages, heads, page_rows), bf16),
            pltpu.VMEM((pages, heads, width), f32),
            pltpu.VMEM((pages, heads, width), f32),
            pltpu.VMEM((pages, heads, width), f32),
            pltpu.VMEM((pages, heads, width), f32),
            pltpu.VMEM((pages, heads, width), f32),
            pltpu.VMEM((PARTS, CORES, part_rows * 3 // 2, width), bf16),
            pltpu.VMEM((window * CORES, part_rows * 3 // 2, width), bf16),
            pltpu.VMEM((chips, part_rows, width), bf16),
            pltpu.VMEM((own_requests,), jnp.int32),
            pltpu.SMEM((CORES, own_requests), jnp.int32),
            pltpu.SMEM((requests + 1,), jnp.int32),
            pltpu.SemaphoreType.DMA((chunks,)),
            pltpu.SemaphoreType.DMA((chunks,)),
            pltpu.SemaphoreType.DMA((3,)),
            pltpu.SemaphoreType.DMA((2,)),
            pltpu.SemaphoreType.DMA((2,)),
            pltpu.SemaphoreType.REGULAR((len(STEPS), 2)),
            pltpu.SemaphoreType.DMA((window * CORES,)),
            pltpu.SemaphoreType.DMA((window * CORES,)),
            pltpu.SemaphoreType.DMA((chips,)),
            pltpu.SemaphoreType.DMA((chips,)),
            pltpu.SemaphoreType.DMA((chips,)),
        ],
        compiler_params=pltpu.CompilerParams(collective_id=0, has_side_effects=True),
    )(queries, lengths, k_cache.reshape(rows, width), v_cache.reshape(rows, width))
    return result.reshape(requests, group, width)


def solution(mesh):
    return jax.shard_map(
        shards,
        mesh=mesh,
        in_specs=(
            P(("group", "sub"), "head", None),
            P(("group", "sub")),
            P(("group", "seq", "sub"), "head", None),
            P(("group", "seq", "sub"), "head", None),
        ),
        out_specs=P("group", ("head", "sub"), None),
        check_vma=False,
    )
```

```python
import functools

import jax
import jax.numpy as jnp
from jax import lax
from jax.experimental import pallas as pl
from jax.experimental.pallas import tpu as pltpu
from jax.sharding import PartitionSpec as P

PAGE = 128
LONGEST = 192
CORES = 2
NEG = -1e30
MESH = pl.DeviceIdType.MESH
STEPS = (1, 2, 4)
PARTS = 4


def rounded(x):
    return x.astype(jnp.bfloat16).astype(jnp.float32)


def kernel(
    chips,
    q_hbm,
    len_hbm,
    k_hbm,
    v_hbm,
    out_ref,
    kbuf,
    vbuf,
    qbuf,
    weight,
    page_max,
    page_sum,
    run_max,
    run_sum,
    run_out,
    sent,
    got,
    final,
    len_vm,
    len_sm,
    start_sm,
    k_sem,
    v_sem,
    in_sem,
    x_send,
    x_recv,
    token,
    r_send,
    r_recv,
    g_send,
    h_send,
    g_recv,
):
    c, s = lax.axis_index("seq"), lax.axis_index("sub")
    own_requests, heads, width = q_hbm.shape
    requests = own_requests * CORES
    group = heads // CORES
    rows = kbuf.shape[0]
    pages = rows // (PAGE * CORES)
    page_rows = PAGE * CORES
    chunks = k_sem.shape[0]
    chunk_rows = rows // chunks
    chunk_pages = pages // chunks
    per_part = requests // PARTS
    reach = got.shape[0] // (2 * CORES)
    far = sum(STEPS) + 1

    def chip(offset):
        return lax.rem(c + (offset + chips), chips)

    def at(offset, core):
        return {"seq": chip(offset), "sub": core}

    barrier = pltpu.get_barrier_semaphore()
    near = [(o, k) for o in (1, -1) for k in range(CORES)]
    for o, k in near:
        pl.semaphore_signal(barrier, inc=1, device_id=at(o, k), device_id_type=MESH)
    pl.semaphore_signal(barrier, inc=1, device_id=at(0, 1 - s), device_id_type=MESH)

    def k_copy(i):
        part = pl.ds(i * chunk_rows, chunk_rows)
        return pltpu.make_async_copy(k_hbm.at[part], kbuf.at[part], k_sem.at[i])

    def v_copy(i):
        part = pl.ds(i * chunk_rows, chunk_rows)
        return pltpu.make_async_copy(v_hbm.at[part], vbuf.at[part], v_sem.at[i])

    own = pl.ds(s * own_requests, own_requests)
    l_out = pltpu.make_async_copy(len_hbm, len_vm, in_sem.at[2])
    l_own = pltpu.make_async_copy(len_hbm, len_sm.at[s], in_sem.at[1])
    q_own = pltpu.make_async_copy(q_hbm, qbuf.at[own], in_sem.at[0])
    l_out.start()
    q_own.start()
    l_own.start()
    for i in range(chunks):
        k_copy(i).start()
    l_out.wait()
    q_own.wait()
    pl.semaphore_wait(barrier, len(near) + 1)
    l_away = pltpu.make_async_remote_copy(
        src_ref=len_vm, dst_ref=len_sm.at[s], send_sem=x_send.at[1], recv_sem=x_recv.at[1],
        device_id=at(0, 1 - s), device_id_type=MESH,
    )
    q_away = pltpu.make_async_remote_copy(
        src_ref=qbuf.at[own], dst_ref=qbuf.at[own], send_sem=x_send.at[0], recv_sem=x_recv.at[0],
        device_id=at(0, 1 - s), device_id_type=MESH,
    )
    l_away.start()
    q_away.start()
    for i in range(chunks):
        v_copy(i).start()

    def signal_level(level):
        for side, o in enumerate((STEPS[level], -STEPS[level])):
            pl.semaphore_signal(token.at[level, side], inc=1, device_id=at(o, s), device_id_type=MESH)

    def wait_level(level):
        for side in range(2):
            pl.semaphore_wait(token.at[level, side], 1)

    signal_level(0)

    l_own.wait()
    l_away.wait()
    starts = []
    total = jnp.int32(0)
    for r in range(requests):
        starts.append(total)
        start_sm[r] = total
        total = total + len_sm[r // own_requests, r % own_requests]
    start_sm[requests] = total
    base = (c * CORES + s) * pages
    owner = jnp.int32(-1)
    for r in range(requests):
        owner = owner + (starts[r] <= base).astype(jnp.int32)
    owners, firsts = [owner], [None]
    for p in range(1, pages):
        begins = start_sm[owner + 1] <= base + p
        owner = jnp.minimum(owner + begins.astype(jnp.int32), requests - 1)
        owners.append(owner)
        firsts.append(begins)

    q_away.wait()
    for i in range(chunks):
        k_copy(i).wait()
        v_copy(i).wait()
    lane_head = lax.rem(lax.broadcasted_iota(jnp.int32, (heads, page_rows), 1), CORES)
    row_head = lax.broadcasted_iota(jnp.int32, (heads, page_rows), 0) // group
    mine = lane_head == row_head
    scale = float(width) ** -0.5
    running = None
    for p in range(pages):
        keys = kbuf[p * page_rows : (p + 1) * page_rows, :]
        values = lax.dot_general(
            qbuf[owners[p]], keys, (((1,), (1,)), ((), ())), preferred_element_type=jnp.float32
        )
        values = jnp.where(mine, values * scale, NEG)
        top = jnp.broadcast_to(jnp.max(values, axis=1, keepdims=True), (heads, width))
        values = jnp.exp(values - jnp.concatenate([top] * CORES, axis=1))
        weight[p] = values.astype(jnp.bfloat16)
        page_max[p] = top
        page_sum[p] = jnp.broadcast_to(jnp.sum(values, axis=1, keepdims=True), (heads, width))
        running = top if p == 0 else jnp.where(firsts[p], top, jnp.maximum(running, top))
        run_max[p] = running

    wait_level(0)
    signal_level(1)

    summed = gathered = None
    for p in range(pages):
        last = jnp.clip(start_sm[owners[p] + 1] - base - 1, 0, pages - 1)
        lift = jnp.exp(page_max[p] - rounded(run_max[last]))
        values = vbuf[p * page_rows : (p + 1) * page_rows, :]
        added = lift * jnp.dot(weight[p], values, preferred_element_type=jnp.float32)
        gathered = added if p == 0 else jnp.where(firsts[p], added, gathered + added)
        run_out[p] = gathered
        added = lift * page_sum[p]
        summed = added if p == 0 else jnp.where(firsts[p], added, summed + added)
        run_sum[p] = summed

    lane = lax.broadcasted_iota(jnp.int32, (heads, width), 1)
    half = lax.rem(lane, width // 2)
    tops, sums, outs = [], [], []
    for r in range(requests):
        begin = jnp.maximum(starts[r] - base, 0)
        end = jnp.minimum(start_sm[r + 1] - base, pages)
        here = end > begin
        last = jnp.clip(end - 1, 0, pages - 1)
        peak = rounded(jnp.where(here, run_max[last], NEG))
        weights = jnp.where(here, run_sum[last], 0.0)
        high = weights.astype(jnp.bfloat16).astype(jnp.float32)
        tops.append(jnp.where(half < 16, peak, jnp.where(half < 32, high, weights - high)))
        outs.append(jnp.where(here, run_out[last], 0.0))

    for j in range(PARTS):
        members = range(j * per_part, (j + 1) * per_part)
        for k in range(CORES):
            cut = slice(k * group, (k + 1) * group)
            numbers = jnp.concatenate([outs[r][cut] for r in members], axis=0)
            lower, upper = (
                jnp.concatenate([tops[r][cut] for r in some], axis=0)
                for some in (members[: per_part // 2], members[per_part // 2 :])
            )
            stats = jnp.where(lane < width // 2, lower, upper)
            sent[j, k] = jnp.concatenate([numbers, stats], axis=0).astype(jnp.bfloat16)

    wait_level(1)
    signal_level(2)

    part_rows = per_part * group
    offsets = [o for n in range(reach, 0, -1) for o in (n, -n)] + [0]

    def part_copy(o, k, n):
        return pltpu.make_async_remote_copy(
            src_ref=sent.at[lax.rem(chip(o), PARTS), k],
            dst_ref=got.at[(reach - o) * CORES + s],
            send_sem=r_send.at[n],
            recv_sem=r_recv.at[(reach - o) * CORES + s],
            device_id=at(o, k),
            device_id_type=MESH,
        )

    def part_arrival(o, k):
        slot = (reach + o) * CORES + k
        return pltpu.make_async_remote_copy(
            src_ref=sent.at[0, 0], dst_ref=got.at[slot], send_sem=r_send.at[0], recv_sem=r_recv.at[slot],
            device_id=at(0, 1 - s), device_id_type=MESH,
        )

    part_copies = []
    for o in offsets:
        for k in range(CORES) if o else (1 - s,):
            part_copies.append(part_copy(o, k, len(part_copies)))
            part_copies[-1].start()
    got[reach * CORES + s] = sent[lax.rem(c, PARTS), s]
    for o in offsets:
        for k in range(CORES) if o else (1 - s,):
            part_arrival(o, k).wait_recv()

    slots = got.shape[0]
    stats = [got[i, part_rows:, :].astype(jnp.float32) for i in range(slots)]
    peak = functools.reduce(jnp.maximum, stats)
    blocks = []
    for t in range(2):
        first = t * width // 2
        numer, denom = 0.0, 0.0
        for i in range(slots):
            lift = jnp.exp(stats[i][:, first : first + 1] - peak[:, first : first + 1])
            part = got[i, t * part_rows // 2 : (t + 1) * part_rows // 2, :]
            numer = numer + lift * part.astype(jnp.float32)
            denom = denom + lift * stats[i]
        denom = denom[:, first + 16 : first + 17] + denom[:, first + 32 : first + 33]
        blocks.append(numer / jnp.where(denom > 0.0, denom, 1.0))
    final[c] = jnp.concatenate(blocks, axis=0).astype(jnp.bfloat16)

    def spread_copy(sem, origin, to):
        return pltpu.make_async_remote_copy(
            src_ref=final.at[origin], dst_ref=final.at[origin], send_sem=sem,
            recv_sem=g_recv.at[origin], device_id={"seq": to, "sub": s}, device_id_type=MESH,
        )

    def arrived(origin):
        spread_copy(g_send.at[0], origin, chip(1)).wait_recv()

    wait_level(2)
    beyond = chips // 2 - far
    direct = [o for n in range(far, 0, -1) for o in (n, -n)]
    for o in (far, -far):
        spread_copy(g_send.at[chip(o)], c, chip(o)).start()
    for to in range(chips):
        ahead = lax.rem(to - c + chips, chips)

        @pl.when(((ahead > 0) & (ahead < far)) | (ahead > chips - far))
        def _():
            spread_copy(g_send.at[to], c, to).start()

    def upward(act):
        for to in range(chips):
            ahead = lax.rem(to - c + chips, chips)

            @pl.when((ahead > 0) & (ahead <= beyond))
            def _():
                act(spread_copy(h_send.at[to], chip(-far), to))

    def downward(act):
        for to in range(chips):
            ahead = lax.rem(to - c + chips, chips)

            @pl.when(ahead > chips - beyond)
            def _():
                act(spread_copy(h_send.at[to], chip(far), to))

    @pl.when(c < chips // 2)
    def _():
        arrived(chip(far))
        downward(lambda copy: copy.start())
        arrived(chip(-far))
        upward(lambda copy: copy.start())

    @pl.when(c >= chips // 2)
    def _():
        arrived(chip(-far))
        upward(lambda copy: copy.start())
        arrived(chip(far))
        downward(lambda copy: copy.start())

    for n in range(1, chips):
        if n not in (far, chips - far):
            arrived(chip(n))

    row_request = lax.broadcasted_iota(jnp.int32, (part_rows, width), 0) // group
    for j in range(PARTS):
        block = None
        for i in range(per_part):
            home = starts[j * per_part + i] // (pages * CORES)
            home = home + lax.rem(j - lax.rem(home, PARTS) + PARTS, PARTS)
            piece = final[lax.rem(home, chips)].astype(jnp.float32)
            block = piece if i == 0 else jnp.where(row_request == i, piece, block)
        out_ref[j * part_rows : (j + 1) * part_rows, :] = block.astype(jnp.bfloat16)

    for n in range(len(part_copies)):
        part_copies[n].wait_send()
    for o in direct:
        spread_copy(g_send.at[chip(o)], c, chip(o)).wait_send()
    upward(lambda copy: copy.wait_send())
    downward(lambda copy: copy.wait_send())


def shards(queries, lengths, k_cache, v_cache):
    chips = lax.axis_size("seq")
    own_requests, heads, width = queries.shape
    tokens, key_heads, _ = k_cache.shape
    requests = own_requests * CORES
    group = heads // key_heads
    rows = tokens * key_heads
    pages = tokens // PAGE
    page_rows = PAGE * key_heads
    span = -(-(LONGEST - 1) // (pages * CORES))
    window = 2 * span + 1
    part_rows = requests // PARTS * group
    chunks = 4
    bf16, f32 = jnp.bfloat16, jnp.float32
    result = pl.pallas_call(
        functools.partial(kernel, chips),
        out_shape=jax.ShapeDtypeStruct((requests * group, width), bf16),
        in_specs=[pl.BlockSpec(memory_space=pl.ANY)] * 4,
        out_specs=pl.BlockSpec(memory_space=pltpu.VMEM),
        scratch_shapes=[
            pltpu.VMEM((rows, width), bf16),
            pltpu.VMEM((rows, width), bf16),
            pltpu.VMEM((requests, heads, width), bf16),
            pltpu.VMEM((pages, heads, page_rows), bf16),
            pltpu.VMEM((pages, heads, width), f32),
            pltpu.VMEM((pages, heads, width), f32),
            pltpu.VMEM((pages, heads, width), f32),
            pltpu.VMEM((pages, heads, width), f32),
            pltpu.VMEM((pages, heads, width), f32),
            pltpu.VMEM((PARTS, CORES, part_rows * 3 // 2, width), bf16),
            pltpu.VMEM((window * CORES, part_rows * 3 // 2, width), bf16),
            pltpu.VMEM((chips, part_rows, width), bf16),
            pltpu.VMEM((own_requests,), jnp.int32),
            pltpu.SMEM((CORES, own_requests), jnp.int32),
            pltpu.SMEM((requests + 1,), jnp.int32),
            pltpu.SemaphoreType.DMA((chunks,)),
            pltpu.SemaphoreType.DMA((chunks,)),
            pltpu.SemaphoreType.DMA((3,)),
            pltpu.SemaphoreType.DMA((2,)),
            pltpu.SemaphoreType.DMA((2,)),
            pltpu.SemaphoreType.REGULAR((len(STEPS), 2)),
            pltpu.SemaphoreType.DMA((window * CORES,)),
            pltpu.SemaphoreType.DMA((window * CORES,)),
            pltpu.SemaphoreType.DMA((chips,)),
            pltpu.SemaphoreType.DMA((chips,)),
            pltpu.SemaphoreType.DMA((chips,)),
        ],
        compiler_params=pltpu.CompilerParams(collective_id=0, has_side_effects=True),
    )(queries, lengths, k_cache.reshape(rows, width), v_cache.reshape(rows, width))
    return result.reshape(requests, group, width)


def solution(mesh):
    return jax.shard_map(
        shards,
        mesh=mesh,
        in_specs=(
            P(("group", "sub"), "head", None),
            P(("group", "sub")),
            P(("group", "seq", "sub"), "head", None),
            P(("group", "seq", "sub"), "head", None),
        ),
        out_specs=P("group", ("head", "sub"), None),
        check_vma=False,
    )
```

```python
import functools

import jax
import jax.numpy as jnp
from jax import lax
from jax.experimental import pallas as pl
from jax.experimental.pallas import tpu as pltpu
from jax.sharding import PartitionSpec as P

PAGE = 128
LONGEST = 192
CORES = 2
NEG = -1e30
MESH = pl.DeviceIdType.MESH
STEPS = (1, 2, 4)
PARTS = 4


def rounded(x):
    return x.astype(jnp.bfloat16).astype(jnp.float32)


def kernel(
    chips,
    q_hbm,
    len_hbm,
    k_hbm,
    v_hbm,
    out_ref,
    kbuf,
    vbuf,
    qbuf,
    weight,
    page_max,
    page_sum,
    run_max,
    run_sum,
    run_out,
    sent,
    got,
    final,
    len_vm,
    len_sm,
    start_sm,
    k_sem,
    v_sem,
    in_sem,
    x_send,
    x_recv,
    token,
    r_send,
    r_recv,
    g_send,
    h_send,
    g_recv,
):
    c, s = lax.axis_index("seq"), lax.axis_index("sub")
    own_requests, heads, width = q_hbm.shape
    requests = own_requests * CORES
    group = heads // CORES
    rows = kbuf.shape[0]
    pages = rows // (PAGE * CORES)
    page_rows = PAGE * CORES
    chunks = k_sem.shape[0]
    chunk_rows = rows // chunks
    chunk_pages = pages // chunks
    slots = requests // 2
    per_part = slots // PARTS
    reach = got.shape[0] // (2 * CORES)
    far = sum(STEPS) + 1

    def chip(offset):
        return lax.rem(c + (offset + chips), chips)

    def at(offset, core):
        return {"seq": chip(offset), "sub": core}

    barrier = pltpu.get_barrier_semaphore()
    near = [(o, k) for o in (1, -1) for k in range(CORES)]
    for o, k in near:
        pl.semaphore_signal(barrier, inc=1, device_id=at(o, k), device_id_type=MESH)
    pl.semaphore_signal(barrier, inc=1, device_id=at(0, 1 - s), device_id_type=MESH)

    def k_copy(i):
        part = pl.ds(i * chunk_rows, chunk_rows)
        return pltpu.make_async_copy(k_hbm.at[part], kbuf.at[part], k_sem.at[i])

    def v_copy(i):
        part = pl.ds(i * chunk_rows, chunk_rows)
        return pltpu.make_async_copy(v_hbm.at[part], vbuf.at[part], v_sem.at[i])

    own = pl.ds(s * own_requests, own_requests)
    l_out = pltpu.make_async_copy(len_hbm, len_vm, in_sem.at[2])
    l_own = pltpu.make_async_copy(len_hbm, len_sm.at[s], in_sem.at[1])
    q_own = pltpu.make_async_copy(q_hbm, qbuf.at[own], in_sem.at[0])
    l_out.start()
    q_own.start()
    l_own.start()
    for i in range(chunks):
        k_copy(i).start()
    l_out.wait()
    q_own.wait()
    pl.semaphore_wait(barrier, len(near) + 1)
    l_away = pltpu.make_async_remote_copy(
        src_ref=len_vm, dst_ref=len_sm.at[s], send_sem=x_send.at[1], recv_sem=x_recv.at[1],
        device_id=at(0, 1 - s), device_id_type=MESH,
    )
    q_away = pltpu.make_async_remote_copy(
        src_ref=qbuf.at[own], dst_ref=qbuf.at[own], send_sem=x_send.at[0], recv_sem=x_recv.at[0],
        device_id=at(0, 1 - s), device_id_type=MESH,
    )
    l_away.start()
    q_away.start()
    for i in range(chunks):
        v_copy(i).start()

    def signal_level(level):
        for side, o in enumerate((STEPS[level], -STEPS[level])):
            pl.semaphore_signal(token.at[level, side], inc=1, device_id=at(o, s), device_id_type=MESH)

    def wait_level(level):
        for side in range(2):
            pl.semaphore_wait(token.at[level, side], 1)

    signal_level(0)

    l_own.wait()
    l_away.wait()
    starts = []
    total = jnp.int32(0)
    for r in range(requests):
        starts.append(total)
        start_sm[r] = total
        total = total + len_sm[r // own_requests, r % own_requests]
    start_sm[requests] = total
    base = (c * CORES + s) * pages
    owner = jnp.int32(-1)
    for r in range(requests):
        owner = owner + (starts[r] <= base).astype(jnp.int32)
    owners, firsts = [owner], [None]
    for p in range(1, pages):
        begins = start_sm[owner + 1] <= base + p
        owner = jnp.minimum(owner + begins.astype(jnp.int32), requests - 1)
        owners.append(owner)
        firsts.append(begins)

    q_away.wait()
    for i in range(chunks):
        k_copy(i).wait()
        v_copy(i).wait()
    lane_head = lax.rem(lax.broadcasted_iota(jnp.int32, (heads, page_rows), 1), CORES)
    row_head = lax.broadcasted_iota(jnp.int32, (heads, page_rows), 0) // group
    mine = lane_head == row_head
    scale = float(width) ** -0.5
    running = None
    for p in range(pages):
        keys = kbuf[p * page_rows : (p + 1) * page_rows, :]
        values = lax.dot_general(
            qbuf[owners[p]], keys, (((1,), (1,)), ((), ())), preferred_element_type=jnp.float32
        )
        values = jnp.where(mine, values * scale, NEG)
        top = jnp.broadcast_to(jnp.max(values, axis=1, keepdims=True), (heads, width))
        values = jnp.exp(values - jnp.concatenate([top] * CORES, axis=1))
        weight[p] = values.astype(jnp.bfloat16)
        page_max[p] = top
        page_sum[p] = jnp.broadcast_to(jnp.sum(values, axis=1, keepdims=True), (heads, width))
        running = top if p == 0 else jnp.where(firsts[p], top, jnp.maximum(running, top))
        run_max[p] = running

    wait_level(0)
    signal_level(1)

    offsets = [o for n in range(reach, 0, -1) for o in (n, -n)] + [0]
    chosen = []
    for o in offsets:
        picks = []
        for i in range(per_part):
            slot = lax.rem(chip(o), PARTS) * per_part + i
            home = start_sm[slot + slots] // (pages * CORES)
            later = lax.rem(chip(o) - home + chips, chips) < PARTS
            r = jnp.where(later, slot + slots, slot)
            begin = jnp.maximum(start_sm[r] - base, 0)
            end = jnp.minimum(start_sm[r + 1] - base, pages)
            picks.append((end > begin, jnp.clip(end - 1, 0, pages - 1)))
        chosen.append(picks)

    summed = gathered = None
    for p in range(pages):
        last = jnp.clip(start_sm[owners[p] + 1] - base - 1, 0, pages - 1)
        lift = jnp.exp(page_max[p] - rounded(run_max[last]))
        values = vbuf[p * page_rows : (p + 1) * page_rows, :]
        added = lift * jnp.dot(weight[p], values, preferred_element_type=jnp.float32)
        gathered = added if p == 0 else jnp.where(firsts[p], added, gathered + added)
        run_out[p] = gathered
        added = lift * page_sum[p]
        summed = added if p == 0 else jnp.where(firsts[p], added, summed + added)
        run_sum[p] = summed

    lane = lax.broadcasted_iota(jnp.int32, (heads, width), 1)
    for n, picks in enumerate(chosen):
        tops, outs = [], []
        for here, last in picks:
            peak = rounded(jnp.where(here, run_max[last], NEG))
            weights = jnp.where(here, run_sum[last], 0.0)
            high = rounded(weights)
            tops.append(jnp.where(lane < 16, peak, jnp.where(lane < 32, high, weights - high)))
            outs.append(jnp.where(here, run_out[last], 0.0))
        for k in range(CORES):
            cut = slice(k * group, (k + 1) * group)
            sent[n, k] = jnp.concatenate([t[cut] for t in outs + tops], axis=0).astype(jnp.bfloat16)

    wait_level(1)
    signal_level(2)

    part_rows = per_part * group

    def part_copy(o, k, n):
        return pltpu.make_async_remote_copy(
            src_ref=sent.at[offsets.index(o), k],
            dst_ref=got.at[(reach - o) * CORES + s],
            send_sem=r_send.at[n],
            recv_sem=r_recv.at[(reach - o) * CORES + s],
            device_id=at(o, k),
            device_id_type=MESH,
        )

    def part_arrival(o, k):
        slot = (reach + o) * CORES + k
        return pltpu.make_async_remote_copy(
            src_ref=sent.at[0, 0], dst_ref=got.at[slot], send_sem=r_send.at[0], recv_sem=r_recv.at[slot],
            device_id=at(0, 1 - s), device_id_type=MESH,
        )

    part_copies = []
    for o in offsets:
        for k in range(CORES) if o else (1 - s,):
            part_copies.append(part_copy(o, k, len(part_copies)))
            part_copies[-1].start()
    got[reach * CORES + s] = sent[len(offsets) - 1, s]
    for o in offsets:
        for k in range(CORES) if o else (1 - s,):
            part_arrival(o, k).wait_recv()

    parts = [got[i].astype(jnp.float32) for i in range(got.shape[0])]
    stats = [part[part_rows:] for part in parts]
    peak = functools.reduce(jnp.maximum, stats)
    numer, denom = 0.0, 0.0
    for part, stat in zip(parts, stats):
        lift = jnp.exp(stat[:, 0:1] - peak[:, 0:1])
        numer = numer + lift * part[:part_rows]
        denom = denom + lift * stat
    denom = denom[:, 16:17] + denom[:, 32:33]
    final[c] = (numer / jnp.where(denom > 0.0, denom, 1.0)).astype(jnp.bfloat16)

    def spread_copy(sem, origin, to):
        return pltpu.make_async_remote_copy(
            src_ref=final.at[origin], dst_ref=final.at[origin], send_sem=sem,
            recv_sem=g_recv.at[origin], device_id={"seq": to, "sub": s}, device_id_type=MESH,
        )

    def arrived(origin):
        spread_copy(g_send.at[0], origin, chip(1)).wait_recv()

    wait_level(2)
    beyond = chips // 2 - far
    direct = [o for n in range(far, 0, -1) for o in (n, -n)]
    for o in (far, -far):
        spread_copy(g_send.at[chip(o)], c, chip(o)).start()
    for to in range(chips):
        ahead = lax.rem(to - c + chips, chips)

        @pl.when(((ahead > 0) & (ahead < far)) | (ahead > chips - far))
        def _():
            spread_copy(g_send.at[to], c, to).start()

    def upward(act):
        for to in range(chips):
            ahead = lax.rem(to - c + chips, chips)

            @pl.when((ahead > 0) & (ahead <= beyond))
            def _():
                act(spread_copy(h_send.at[to], chip(-far), to))

    def downward(act):
        for to in range(chips):
            ahead = lax.rem(to - c + chips, chips)

            @pl.when(ahead > chips - beyond)
            def _():
                act(spread_copy(h_send.at[to], chip(far), to))

    @pl.when(c < chips // 2)
    def _():
        arrived(chip(far))
        downward(lambda copy: copy.start())
        arrived(chip(-far))
        upward(lambda copy: copy.start())

    @pl.when(c >= chips // 2)
    def _():
        arrived(chip(-far))
        upward(lambda copy: copy.start())
        arrived(chip(far))
        downward(lambda copy: copy.start())

    for n in range(1, chips):
        if n not in (far, chips - far):
            arrived(chip(n))

    row_request = lax.broadcasted_iota(jnp.int32, (part_rows, width), 0) // group
    for t in range(requests // per_part):
        block = None
        for i in range(per_part):
            home = starts[t * per_part + i] // (pages * CORES)
            home = home + lax.rem(t % PARTS - lax.rem(home, PARTS) + PARTS, PARTS)
            piece = final[lax.rem(home, chips)].astype(jnp.float32)
            block = piece if i == 0 else jnp.where(row_request == i, piece, block)
        out_ref[t * part_rows : (t + 1) * part_rows, :] = block.astype(jnp.bfloat16)

    for n in range(len(part_copies)):
        part_copies[n].wait_send()
    for o in direct:
        spread_copy(g_send.at[chip(o)], c, chip(o)).wait_send()
    upward(lambda copy: copy.wait_send())
    downward(lambda copy: copy.wait_send())


def shards(queries, lengths, k_cache, v_cache):
    chips = lax.axis_size("seq")
    own_requests, heads, width = queries.shape
    tokens, key_heads, _ = k_cache.shape
    requests = own_requests * CORES
    group = heads // key_heads
    rows = tokens * key_heads
    pages = tokens // PAGE
    page_rows = PAGE * key_heads
    span = -(-(LONGEST - 1) // (pages * CORES))
    window = 2 * span + 1
    part_rows = requests // 2 // PARTS * group
    elsewhere = -(-(chips * pages * CORES - PARTS * pages * CORES - LONGEST + 1) // LONGEST)
    assert requests - elsewhere <= requests // 2
    chunks = 4
    bf16, f32 = jnp.bfloat16, jnp.float32
    result = pl.pallas_call(
        functools.partial(kernel, chips),
        out_shape=jax.ShapeDtypeStruct((requests * group, width), bf16),
        in_specs=[pl.BlockSpec(memory_space=pl.ANY)] * 4,
        out_specs=pl.BlockSpec(memory_space=pltpu.VMEM),
        scratch_shapes=[
            pltpu.VMEM((rows, width), bf16),
            pltpu.VMEM((rows, width), bf16),
            pltpu.VMEM((requests, heads, width), bf16),
            pltpu.VMEM((pages, heads, page_rows), bf16),
            pltpu.VMEM((pages, heads, width), f32),
            pltpu.VMEM((pages, heads, width), f32),
            pltpu.VMEM((pages, heads, width), f32),
            pltpu.VMEM((pages, heads, width), f32),
            pltpu.VMEM((pages, heads, width), f32),
            pltpu.VMEM((window, CORES, 2 * part_rows, width), bf16),
            pltpu.VMEM((window * CORES, 2 * part_rows, width), bf16),
            pltpu.VMEM((chips, part_rows, width), bf16),
            pltpu.VMEM((own_requests,), jnp.int32),
            pltpu.SMEM((CORES, own_requests), jnp.int32),
            pltpu.SMEM((requests + 1,), jnp.int32),
            pltpu.SemaphoreType.DMA((chunks,)),
            pltpu.SemaphoreType.DMA((chunks,)),
            pltpu.SemaphoreType.DMA((3,)),
            pltpu.SemaphoreType.DMA((2,)),
            pltpu.SemaphoreType.DMA((2,)),
            pltpu.SemaphoreType.REGULAR((len(STEPS), 2)),
            pltpu.SemaphoreType.DMA((window * CORES,)),
            pltpu.SemaphoreType.DMA((window * CORES,)),
            pltpu.SemaphoreType.DMA((chips,)),
            pltpu.SemaphoreType.DMA((chips,)),
            pltpu.SemaphoreType.DMA((chips,)),
        ],
        compiler_params=pltpu.CompilerParams(collective_id=0, has_side_effects=True),
    )(queries, lengths, k_cache.reshape(rows, width), v_cache.reshape(rows, width))
    return result.reshape(requests, group, width)


def solution(mesh):
    return jax.shard_map(
        shards,
        mesh=mesh,
        in_specs=(
            P(("group", "sub"), "head", None),
            P(("group", "sub")),
            P(("group", "seq", "sub"), "head", None),
            P(("group", "seq", "sub"), "head", None),
        ),
        out_specs=P("group", ("head", "sub"), None),
        check_vma=False,
    )
```

```python
import functools

import jax
import jax.numpy as jnp
from jax import lax
from jax.experimental import pallas as pl
from jax.experimental.pallas import tpu as pltpu
from jax.sharding import PartitionSpec as P

PAGE = 128
LONGEST = 192
CORES = 2
NEG = -1e30
MESH = pl.DeviceIdType.MESH
STEPS = (1, 2, 4)
PARTS = 4


def rounded(x):
    return x.astype(jnp.bfloat16).astype(jnp.float32)


def kernel(
    chips,
    q_hbm,
    len_hbm,
    k_hbm,
    v_hbm,
    out_ref,
    kbuf,
    vbuf,
    qbuf,
    weight,
    page_max,
    page_sum,
    run_max,
    run_sum,
    run_out,
    sent,
    got,
    final,
    mixed,
    len_vm,
    len_sm,
    start_sm,
    k_sem,
    v_sem,
    in_sem,
    x_send,
    x_recv,
    token,
    r_send,
    r_recv,
    g_send,
    h_send,
    g_recv,
):
    c, s = lax.axis_index("seq"), lax.axis_index("sub")
    own_requests, heads, width = q_hbm.shape
    requests = own_requests * CORES
    group = heads // CORES
    rows = kbuf.shape[0]
    pages = rows // (PAGE * CORES)
    page_rows = PAGE * CORES
    chunks = k_sem.shape[0]
    chunk_rows = rows // chunks
    chunk_pages = pages // chunks
    slots = requests // 2
    per_part = slots // PARTS
    reach = got.shape[0] // (2 * CORES)
    far = sum(STEPS) + 1

    def chip(offset):
        return lax.rem(c + (offset + chips), chips)

    def at(offset, core):
        return {"seq": chip(offset), "sub": core}

    barrier = pltpu.get_barrier_semaphore()
    near = [(o, k) for o in (1, -1) for k in range(CORES)]
    for o, k in near:
        pl.semaphore_signal(barrier, inc=1, device_id=at(o, k), device_id_type=MESH)
    pl.semaphore_signal(barrier, inc=1, device_id=at(0, 1 - s), device_id_type=MESH)

    def k_copy(i):
        part = pl.ds(i * chunk_rows, chunk_rows)
        return pltpu.make_async_copy(k_hbm.at[part], kbuf.at[part], k_sem.at[i])

    def v_copy(i):
        part = pl.ds(i * chunk_rows, chunk_rows)
        return pltpu.make_async_copy(v_hbm.at[part], vbuf.at[part], v_sem.at[i])

    own = pl.ds(s * own_requests, own_requests)
    l_out = pltpu.make_async_copy(len_hbm, len_vm, in_sem.at[2])
    l_own = pltpu.make_async_copy(len_hbm, len_sm.at[s], in_sem.at[1])
    q_own = pltpu.make_async_copy(q_hbm, qbuf.at[own], in_sem.at[0])
    l_out.start()
    q_own.start()
    l_own.start()
    for i in range(chunks):
        k_copy(i).start()
    l_out.wait()
    q_own.wait()
    pl.semaphore_wait(barrier, len(near) + 1)
    l_away = pltpu.make_async_remote_copy(
        src_ref=len_vm, dst_ref=len_sm.at[s], send_sem=x_send.at[1], recv_sem=x_recv.at[1],
        device_id=at(0, 1 - s), device_id_type=MESH,
    )
    q_away = pltpu.make_async_remote_copy(
        src_ref=qbuf.at[own], dst_ref=qbuf.at[own], send_sem=x_send.at[0], recv_sem=x_recv.at[0],
        device_id=at(0, 1 - s), device_id_type=MESH,
    )
    l_away.start()
    q_away.start()
    for i in range(chunks):
        v_copy(i).start()

    def signal_level(level):
        for side, o in enumerate((STEPS[level], -STEPS[level])):
            pl.semaphore_signal(token.at[level, side], inc=1, device_id=at(o, s), device_id_type=MESH)

    def wait_level(level):
        for side in range(2):
            pl.semaphore_wait(token.at[level, side], 1)

    signal_level(0)

    l_own.wait()
    l_away.wait()
    starts = []
    total = jnp.int32(0)
    for r in range(requests):
        starts.append(total)
        start_sm[r] = total
        total = total + len_sm[r // own_requests, r % own_requests]
    start_sm[requests] = total
    base = (c * CORES + s) * pages
    owner = jnp.int32(-1)
    for r in range(requests):
        owner = owner + (starts[r] <= base).astype(jnp.int32)
    owners, firsts = [owner], [None]
    for p in range(1, pages):
        begins = start_sm[owner + 1] <= base + p
        owner = jnp.minimum(owner + begins.astype(jnp.int32), requests - 1)
        owners.append(owner)
        firsts.append(begins)

    q_away.wait()
    for i in range(chunks):
        k_copy(i).wait()
        v_copy(i).wait()
    lane_head = lax.rem(lax.broadcasted_iota(jnp.int32, (heads, page_rows), 1), CORES)
    row_head = lax.broadcasted_iota(jnp.int32, (heads, page_rows), 0) // group
    mine = lane_head == row_head
    scale = float(width) ** -0.5
    running = None
    for p in range(pages):
        keys = kbuf[p * page_rows : (p + 1) * page_rows, :]
        values = lax.dot_general(
            qbuf[owners[p]], keys, (((1,), (1,)), ((), ())), preferred_element_type=jnp.float32
        )
        values = jnp.where(mine, values * scale, NEG)
        top = jnp.broadcast_to(jnp.max(values, axis=1, keepdims=True), (heads, width))
        values = jnp.exp(values - jnp.concatenate([top] * CORES, axis=1))
        weight[p] = values.astype(jnp.bfloat16)
        page_max[p] = top
        page_sum[p] = jnp.broadcast_to(jnp.sum(values, axis=1, keepdims=True), (heads, width))
        running = top if p == 0 else jnp.where(firsts[p], top, jnp.maximum(running, top))
        run_max[p] = running

    wait_level(0)
    signal_level(1)

    offsets = [o for n in range(reach, 0, -1) for o in (n, -n)] + [0]
    chosen = []
    for o in offsets:
        picks = []
        for i in range(per_part):
            slot = lax.rem(chip(o), PARTS) * per_part + i
            home = start_sm[slot + slots] // (pages * CORES)
            later = lax.rem(chip(o) - home + chips, chips) < PARTS
            r = jnp.where(later, slot + slots, slot)
            begin = jnp.maximum(start_sm[r] - base, 0)
            end = jnp.minimum(start_sm[r + 1] - base, pages)
            picks.append((end > begin, jnp.clip(end - 1, 0, pages - 1)))
        chosen.append(picks)

    summed = gathered = None
    for p in range(pages):
        last = jnp.clip(start_sm[owners[p] + 1] - base - 1, 0, pages - 1)
        lift = jnp.exp(page_max[p] - rounded(run_max[last]))
        values = vbuf[p * page_rows : (p + 1) * page_rows, :]
        added = lift * jnp.dot(weight[p], values, preferred_element_type=jnp.float32)
        gathered = added if p == 0 else jnp.where(firsts[p], added, gathered + added)
        run_out[p] = gathered
        added = lift * page_sum[p]
        summed = added if p == 0 else jnp.where(firsts[p], added, summed + added)
        run_sum[p] = summed

    lane = lax.broadcasted_iota(jnp.int32, (heads, width), 1)
    for n, picks in enumerate(chosen):
        tops, outs = [], []
        for here, last in picks:
            peak = rounded(jnp.where(here, run_max[last], NEG))
            weights = jnp.where(here, run_sum[last], 0.0)
            high = rounded(weights)
            tops.append(jnp.where(lane < 16, peak, jnp.where(lane < 32, high, weights - high)))
            outs.append(jnp.where(here, run_out[last], 0.0))
        for k in range(CORES):
            cut = slice(k * group, (k + 1) * group)
            sent[n, k] = jnp.concatenate([t[cut] for t in outs + tops], axis=0).astype(jnp.bfloat16)

    wait_level(1)
    signal_level(2)

    part_rows = per_part * group

    def part_copy(o, k, n):
        return pltpu.make_async_remote_copy(
            src_ref=sent.at[offsets.index(o), k],
            dst_ref=got.at[(reach - o) * CORES + s],
            send_sem=r_send.at[n],
            recv_sem=r_recv.at[(reach - o) * CORES + s],
            device_id=at(o, k),
            device_id_type=MESH,
        )

    def part_arrival(o, k):
        slot = (reach + o) * CORES + k
        return pltpu.make_async_remote_copy(
            src_ref=sent.at[0, 0], dst_ref=got.at[slot], send_sem=r_send.at[0], recv_sem=r_recv.at[slot],
            device_id=at(0, 1 - s), device_id_type=MESH,
        )

    part_copies = []
    for o in offsets:
        for k in range(CORES) if o else (1 - s,):
            part_copies.append(part_copy(o, k, len(part_copies)))
            part_copies[-1].start()
    got[reach * CORES + s] = sent[len(offsets) - 1, s]
    for o in offsets:
        for k in range(CORES) if o else (1 - s,):
            part_arrival(o, k).wait_recv()

    parts = [got[i].astype(jnp.float32) for i in range(got.shape[0])]
    stats = [part[part_rows:] for part in parts]
    peak = functools.reduce(jnp.maximum, stats)
    numer, denom = 0.0, 0.0
    for part, stat in zip(parts, stats):
        lift = jnp.exp(stat[:, 0:1] - peak[:, 0:1])
        numer = numer + lift * part[:part_rows]
        denom = denom + lift * stat
    denom = denom[:, 16:17] + denom[:, 32:33]
    final[c] = (numer / jnp.where(denom > 0.0, denom, 1.0)).astype(jnp.bfloat16)

    def spread_copy(sem, origin, to):
        return pltpu.make_async_remote_copy(
            src_ref=final.at[origin], dst_ref=final.at[origin], send_sem=sem,
            recv_sem=g_recv.at[origin], device_id={"seq": to, "sub": s}, device_id_type=MESH,
        )

    def arrived(origin):
        spread_copy(g_send.at[0], origin, chip(1)).wait_recv()

    wait_level(2)
    direct = [o for n in range(far, 0, -1) for o in (n, -n)]
    for o in (far, -far):
        spread_copy(g_send.at[chip(o)], c, chip(o)).start()
    for to in range(chips):
        ahead = lax.rem(to - c + chips, chips)

        @pl.when(((ahead > 0) & (ahead < far)) | (ahead > chips - far))
        def _():
            spread_copy(g_send.at[to], c, to).start()

    half = far // 2
    row_request = lax.broadcasted_iota(jnp.int32, (part_rows, width), 0) // group

    def mixed_copy(side, to):
        place = (1 + side) * chips + c
        return pltpu.make_async_remote_copy(
            src_ref=mixed.at[side], dst_ref=final.at[place], send_sem=h_send.at[to],
            recv_sem=g_recv.at[place], device_id={"seq": to, "sub": s}, device_id_type=MESH,
        )

    def relay(side):
        way = 1 - 2 * side
        nearer, away = chip(-way * half), chip(-way * far)
        arrived(nearer)
        arrived(away)
        pick = None
        for i in range(per_part):
            slot = lax.rem(c, PARTS) * per_part + i
            count = jnp.int32(0)
            for r in (slot, slot + slots):
                home = start_sm[r] // (pages * CORES)
                count = count + (lax.rem(nearer - home + chips, chips) < PARTS).astype(jnp.int32)
            pick = count if i == 0 else jnp.where(row_request == i, count, pick)
        block = jnp.where(
            jnp.broadcast_to(pick, (part_rows, width)) > 0,
            final[nearer].astype(jnp.float32),
            final[away].astype(jnp.float32),
        )
        mixed[side] = block.astype(jnp.bfloat16)
        for to in range(chips):
            ahead = lax.rem(way * (to - c) + chips, chips)

            @pl.when((ahead > half) & (ahead <= far))
            def _():
                mixed_copy(side, to).start()

    @pl.when(c < chips // 2)
    def _():
        relay(1)
        relay(0)

    @pl.when(c >= chips // 2)
    def _():
        relay(0)
        relay(1)

    for n in range(1, far + 1):
        if n not in (half, far):
            arrived(chip(n))
            arrived(chip(-n))
    for n in range(half + 1, far + 1):
        arrived(chips + chip(-n))
        arrived(2 * chips + chip(n))

    for t in range(requests // per_part):
        block = None
        for i in range(per_part):
            home = starts[t * per_part + i] // (pages * CORES)
            home = home + lax.rem(t % PARTS - lax.rem(home, PARTS) + PARTS, PARTS)
            home = lax.rem(home, chips)
            ahead = lax.rem(c - home + chips, chips)
            behind = chips - ahead
            above = home + jnp.where(ahead <= far + half, half, far)
            below = home + chips - jnp.where(behind <= far + half, half, far)
            place = jnp.where(
                ahead <= 2 * far, chips + lax.rem(above, chips), 2 * chips + lax.rem(below, chips)
            )
            place = jnp.where((ahead <= far) | (behind <= far), home, place)
            piece = final[place].astype(jnp.float32)
            block = piece if i == 0 else jnp.where(row_request == i, piece, block)
        out_ref[t * part_rows : (t + 1) * part_rows, :] = block.astype(jnp.bfloat16)

    for n in range(len(part_copies)):
        part_copies[n].wait_send()
    for o in direct:
        spread_copy(g_send.at[chip(o)], c, chip(o)).wait_send()
    for n in range(half + 1, far + 1):
        mixed_copy(0, chip(n)).wait_send()
        mixed_copy(1, chip(-n)).wait_send()


def shards(queries, lengths, k_cache, v_cache):
    chips = lax.axis_size("seq")
    own_requests, heads, width = queries.shape
    tokens, key_heads, _ = k_cache.shape
    requests = own_requests * CORES
    group = heads // key_heads
    rows = tokens * key_heads
    pages = tokens // PAGE
    page_rows = PAGE * key_heads
    span = -(-(LONGEST - 1) // (pages * CORES))
    window = 2 * span + 1
    part_rows = requests // 2 // PARTS * group
    elsewhere = -(-(chips * pages * CORES - PARTS * pages * CORES - LONGEST + 1) // LONGEST)
    assert requests - elsewhere <= requests // 2
    chunks = 4
    bf16, f32 = jnp.bfloat16, jnp.float32
    result = pl.pallas_call(
        functools.partial(kernel, chips),
        out_shape=jax.ShapeDtypeStruct((requests * group, width), bf16),
        in_specs=[pl.BlockSpec(memory_space=pl.ANY)] * 4,
        out_specs=pl.BlockSpec(memory_space=pltpu.VMEM),
        scratch_shapes=[
            pltpu.VMEM((rows, width), bf16),
            pltpu.VMEM((rows, width), bf16),
            pltpu.VMEM((requests, heads, width), bf16),
            pltpu.VMEM((pages, heads, page_rows), bf16),
            pltpu.VMEM((pages, heads, width), f32),
            pltpu.VMEM((pages, heads, width), f32),
            pltpu.VMEM((pages, heads, width), f32),
            pltpu.VMEM((pages, heads, width), f32),
            pltpu.VMEM((pages, heads, width), f32),
            pltpu.VMEM((window, CORES, 2 * part_rows, width), bf16),
            pltpu.VMEM((window * CORES, 2 * part_rows, width), bf16),
            pltpu.VMEM((3 * chips, part_rows, width), bf16),
            pltpu.VMEM((2, part_rows, width), bf16),
            pltpu.VMEM((own_requests,), jnp.int32),
            pltpu.SMEM((CORES, own_requests), jnp.int32),
            pltpu.SMEM((requests + 1,), jnp.int32),
            pltpu.SemaphoreType.DMA((chunks,)),
            pltpu.SemaphoreType.DMA((chunks,)),
            pltpu.SemaphoreType.DMA((3,)),
            pltpu.SemaphoreType.DMA((2,)),
            pltpu.SemaphoreType.DMA((2,)),
            pltpu.SemaphoreType.REGULAR((len(STEPS), 2)),
            pltpu.SemaphoreType.DMA((window * CORES,)),
            pltpu.SemaphoreType.DMA((window * CORES,)),
            pltpu.SemaphoreType.DMA((chips,)),
            pltpu.SemaphoreType.DMA((chips,)),
            pltpu.SemaphoreType.DMA((3 * chips,)),
        ],
        compiler_params=pltpu.CompilerParams(collective_id=0, has_side_effects=True),
    )(queries, lengths, k_cache.reshape(rows, width), v_cache.reshape(rows, width))
    return result.reshape(requests, group, width)


def solution(mesh):
    return jax.shard_map(
        shards,
        mesh=mesh,
        in_specs=(
            P(("group", "sub"), "head", None),
            P(("group", "sub")),
            P(("group", "seq", "sub"), "head", None),
            P(("group", "seq", "sub"), "head", None),
        ),
        out_specs=P("group", ("head", "sub"), None),
        check_vma=False,
    )
```
